32 devices in a mesh: expert: 2 (over core), task: 4 (over y, x), shard: 4 (over z).
Axes of the slice: x: 2, y: 2, z: 4, core: 2. Of those that a mesh axis runs over, the one named last changes fastest.
Arguments:
- weights: bfloat16 [4, 2, 8192, 2048], P('task', None, ('expert', 'shard')), may hold values from -6 to 6
- fisher: bfloat16 [4, 2, 8192, 2048], P('task', None, ('expert', 'shard')), may hold values from 0.049804688 to 5
- base_weights: bfloat16 [2, 8192, 2048], P('expert', 'task', 'shard'), may hold values from -6 to 6
- tile_list: int32 [4, 2, 8, 4], P('task'), may hold values from 0 to 7, as said below
- tile_count: int32 [4, 2, 8], P('task'), may hold values from 0 to 4, as said below
Outputs:
- merged: bfloat16 [2, 8192, 2048], P('expert', 'task', 'shard')
The draws below stay inside these ranges and needn't reach their ends.
Inputs may be any that keep to these rules, and one draw needn't show every extreme that they name: `tile_list`: for each fine-fit, expert and row block the first tile_count entries are distinct tiles of the block, numbered 0 to 7, in ascending order; the remaining entries are 0. `tile_count`: 4 is reached, and for each fine-fit some expert has 4 in every row block.
All inputs are finite; a program needn't handle non-finite values.
Results may differ from the reference program's by a relative error of at most 0.006.
Values may be sent and summed in bfloat16 or wider, within the bound.
A program may use at most 128 MiB of HBM per device.

```python
import math
import jax
import jax.numpy as jnp
from jax import lax

ROWS = 8192
COLS = 2048
TILE = 128
EXPERTS = 2
TASKS = 4
BLOCKS = 8
TPB = 8
CAP = 4


def tile_plan(key):
    base_key = jax.random.fold_in(key, 7)
    key_count, key_full, key_order = jax.random.split(base_key, 3)
    counts = jax.random.randint(key_count, (TASKS, EXPERTS, BLOCKS), 0, CAP + 1)
    full_expert = jax.random.randint(key_full, (TASKS,), 0, EXPERTS)
    is_full = jnp.arange(EXPERTS)[None, :, None] == full_expert[:, None, None]
    counts = jnp.where(is_full, CAP, counts).astype(jnp.int32)
    scores = jax.random.randint(key_order, (TASKS, EXPERTS, BLOCKS, TPB), 0, 1 << 20)
    scores = scores * TPB + jnp.arange(TPB)[None, None, None, :]
    chosen = jnp.argsort(scores, axis=-1)[..., :CAP]
    slot_live = jnp.arange(CAP)[None, None, None, :] < counts[..., None]
    marked = jnp.sort(jnp.where(slot_live, chosen, TPB), axis=-1)
    listed = jnp.where(marked == TPB, 0, marked).astype(jnp.int32)
    return (listed, counts)


def draw_tile_list(key, part):
    return tile_plan(key)[0]


def draw_tile_count(key, part):
    return tile_plan(key)[1]


def shard_levels(stream_key, shape, cuts, smallest, high):
    loudness, own = 1.0, jax.random.fold_in(stream_key, 6)
    for axis_at, blocks in cuts:
        steps = jnp.exp(jax.random.uniform(jax.random.fold_in(own, axis_at), (blocks,), jnp.float32, smallest / len(cuts), high / len(cuts)))
        loudness = loudness * jnp.repeat(steps, shape[axis_at] // blocks).reshape([-1 if axis == axis_at else 1 for axis in range(len(shape))])
    return loudness


def noise(rng, shape, scale, limit, cuts=(), kind=jnp.bfloat16):
    result = jax.random.normal(rng, shape, jnp.float32) * scale
    if len(cuts) > 0:
        result = shard_levels(rng, shape, cuts, -0.22, 0.18) * result
    return jnp.clip(result, min=-limit, max=limit).astype(kind)


def setup_inputs(seed: int = 0) -> dict:
    splits = jax.random.split(jax.random.key(seed), 6)
    weights = noise(splits[0], (TASKS, EXPERTS, ROWS, COLS), 1.0, 6.0, ((0, 4), (2, 8)))
    fisher = jnp.clip(jnp.exp(math.log(5.0) - 4.609084 * jax.random.uniform(splits[1], (TASKS, EXPERTS, ROWS, COLS), jnp.float32) ** shard_levels(splits[1], (TASKS, EXPERTS, ROWS, COLS), ((0, 4), (2, 8)), -0.2, 0.2)), 0.049804688, 5.0).astype(jnp.bfloat16)
    base_weights = noise(splits[2], (EXPERTS, ROWS, COLS), 1.0, 6.0, ((0, 2), (1, 4), (2, 4)))
    tile_list = draw_tile_list(jax.random.fold_in(splits[5], 71), 0)
    tile_count = draw_tile_count(jax.random.fold_in(splits[5], 71), 0)
    return dict(weights=weights, fisher=fisher, base_weights=base_weights, tile_list=tile_list, tile_count=tile_count)


PRIOR_WEIGHT = 0.5


def reference(weights, fisher, base_weights, tile_list, tile_count):
    numerator = jnp.zeros((EXPERTS, ROWS, COLS), jnp.float32)
    denominator = jnp.zeros((EXPERTS, ROWS, COLS), jnp.float32)
    for task_index in range(TASKS):
        slot_live = jnp.arange(CAP, dtype=jnp.int32)[None, None, :] < tile_count[task_index][:, :, None]
        matches = (tile_list[task_index][:, :, :, None] == jnp.arange(TPB, dtype=jnp.int32)[None, None, None, :]) & slot_live[:, :, :, None]
        kept_tiles = jnp.any(matches, axis=2).reshape(EXPERTS, BLOCKS * TPB).astype(jnp.float32)
        row_mask = jnp.repeat(kept_tiles, TILE, axis=1)[:, :, None]
        fisher_now = fisher[task_index].astype(jnp.float32) * row_mask
        term = (fisher_now * weights[task_index].astype(jnp.float32)).astype(jnp.bfloat16)
        term = lax.optimization_barrier(term)
        share = fisher_now.astype(jnp.bfloat16)
        share = lax.optimization_barrier(share)
        numerator = numerator + term.astype(jnp.float32)
        denominator = denominator + share.astype(jnp.float32)
    merged = (numerator + PRIOR_WEIGHT * base_weights.astype(jnp.float32)) / (denominator + PRIOR_WEIGHT)
    return merged.astype(jnp.bfloat16)
```

```python
import functools

import jax
import jax.numpy as jnp
from jax import lax
from jax.experimental import pallas as pl
from jax.experimental.pallas import tpu as pltpu
from jax.sharding import PartitionSpec as P

TILE = 128
PRIOR_WEIGHT = 0.5
DIRECT = 32
MESH = pl.DeviceIdType.MESH


def pack_body(ids, live, weights, fisher, packed):
    expert, slot = pl.program_id(0), pl.program_id(1)
    kept = live[expert * pl.num_programs(1) + slot].astype(jnp.float32)
    pieces, width = packed.shape[1], packed.shape[-1]
    for piece in range(pieces):
        lanes = pl.ds(piece * width, width)
        share = fisher[0, :, lanes].astype(jnp.float32) * kept
        term = share * weights[0, :, lanes].astype(jnp.float32)
        packed[0, piece, 0, 0] = term.astype(jnp.bfloat16)
        packed[0, piece, 1, 0] = share.astype(jnp.bfloat16)


def pack(ids, live, weights, fisher, pieces):
    experts, rows, columns = weights.shape
    cap = ids.shape[0] // experts
    width = columns // pieces
    tile = pl.BlockSpec(
        (1, TILE, columns), lambda e, k, ids, live: (e, ids[e * cap + k], 0)
    )
    return pl.pallas_call(
        pack_body,
        out_shape=jax.ShapeDtypeStruct(
            (experts, pieces, 2, cap, TILE, width), jnp.bfloat16
        ),
        grid_spec=pltpu.PrefetchScalarGridSpec(
            num_scalar_prefetch=2,
            grid=(experts, cap),
            in_specs=[tile, tile],
            out_specs=pl.BlockSpec(
                (1, pieces, 2, 1, TILE, width), lambda e, k, ids, live: (e, 0, 0, k, 0, 0)
            ),
        ),
        name="pack",
    )(ids, live, weights, fisher)


def exchange_body(sizes, packed, received, send_sem, recv_sem, own_sem):
    experts, tasks, shards = sizes
    blocks = experts * shards
    group = blocks // tasks
    expert, task, shard = (lax.axis_index(a) for a in ("expert", "task", "shard"))
    block = expert * shards + shard
    owner = block // group
    place = block % group
    is_own = owner == task
    order = [(de, ds) for ds in range(shards - 1, -1, -1) for de in range(experts)]

    def outgoing(de, ds):
        to_expert = lax.rem(expert + de, experts)
        to_shard = lax.rem(shard + ds, shards)
        return pltpu.make_async_remote_copy(
            src_ref=packed.at[to_expert, to_shard],
            dst_ref=received.at[task, place],
            send_sem=send_sem.at[de, ds],
            recv_sem=recv_sem.at[task, place],
            device_id=(to_expert, owner, to_shard),
            device_id_type=MESH,
        )

    own = pltpu.make_async_copy(
        packed.at[expert, shard], received.at[task, place], own_sem
    )
    for de, ds in order:
        if (de, ds) == (0, 0):
            pl.when(is_own)(own.start)
            pl.when(jnp.logical_not(is_own))(outgoing(de, ds).start)
        else:
            outgoing(de, ds).start()
    for from_task in range(tasks):
        for at in range(group):
            local = jnp.logical_and(is_own, jnp.logical_and(task == from_task, place == at))
            arriving = pltpu.make_async_remote_copy(
                src_ref=packed.at[0, 0],
                dst_ref=received.at[from_task, at],
                send_sem=send_sem.at[0, 0],
                recv_sem=recv_sem.at[from_task, at],
                device_id=(lax.rem(expert + 1, experts), task, shard),
                device_id_type=MESH,
            )
            pl.when(jnp.logical_not(local))(arriving.wait_recv)
    for de, ds in order:
        if (de, ds) == (0, 0):
            pl.when(is_own)(own.wait)
            pl.when(jnp.logical_not(is_own))(outgoing(de, ds).wait_send)
        else:
            outgoing(de, ds).wait_send()


def exchange(packed, sizes):
    experts, tasks, shards = sizes
    group = experts * shards // tasks
    return pl.pallas_call(
        functools.partial(exchange_body, sizes),
        out_shape=jax.ShapeDtypeStruct((tasks, group) + packed.shape[2:], packed.dtype),
        in_specs=[pl.BlockSpec(memory_space=pl.ANY)],
        out_specs=pl.BlockSpec(memory_space=pl.ANY),
        scratch_shapes=[
            pltpu.SemaphoreType.DMA((experts, shards)),
            pltpu.SemaphoreType.DMA((tasks, group)),
            pltpu.SemaphoreType.DMA,
        ],
        compiler_params=pltpu.CompilerParams(has_side_effects=True),
        name="exchange",
    )(packed)


def merge_body(tasks, slots, live, *refs):
    parts, base, merged = refs[:tasks], refs[tasks], refs[tasks + 1]
    at = pl.program_id(0) * pl.num_programs(1) + pl.program_id(1)
    count = pl.num_programs(0) * pl.num_programs(1)
    numerator = PRIOR_WEIGHT * base[...].astype(jnp.float32)
    denominator = jnp.full(base.shape, PRIOR_WEIGHT, jnp.float32)
    for task, part in enumerate(parts):
        kept = live[task * count + at].astype(jnp.float32)
        numerator += part[0, 0, 0, 0].astype(jnp.float32) * kept
        denominator += part[0, 0, 1, 0].astype(jnp.float32) * kept
    merged[...] = (numerator / denominator).astype(jnp.bfloat16)


def merge(slots, live, received, base):
    tasks, group, _, _, _, width = received.shape
    per_block = slots.shape[0] // (tasks * group)

    def part(task):
        return pl.BlockSpec(
            (1, 1, 2, 1, TILE, width),
            lambda g, j, slots, live: (
                task, g, 0, slots[(task * group + g) * per_block + j], 0, 0
            ),
        )

    rows = pl.BlockSpec((TILE, width), lambda g, j, slots, live: (g * per_block + j, 0))
    return pl.pallas_call(
        functools.partial(merge_body, tasks),
        out_shape=jax.ShapeDtypeStruct(base.shape, jnp.bfloat16),
        grid_spec=pltpu.PrefetchScalarGridSpec(
            num_scalar_prefetch=2,
            grid=(group, per_block),
            in_specs=[part(task) for task in range(tasks)] + [rows],
            out_specs=rows,
        ),
        name="merge",
    )(slots, live, *([received] * tasks), base)


def mesh_copy(source, target, send_sem, recv_sem, device):
    return pltpu.make_async_remote_copy(
        src_ref=source, dst_ref=target, send_sem=send_sem, recv_sem=recv_sem,
        device_id=device, device_id_type=MESH,
    )


def fused_body(
    plan, plan_hbm, weights, fisher, base, merged,
    w_buf, f_buf, packed, gathered, sums, direct, far, base_buf, out_buf,
    plans, tables, slots, live,
    in_sem, base_sem, out_sem, p_send, p_recv, table_sem,
    g_send, g_recv, g_own, n_send, n_recv, n_own, s_send, s_recv,
):
    expert, task, shard = (lax.axis_index(a) for a in ("expert", "task", "shard"))
    x, y, half = task % 2, task // 2, shard // 2
    cap = packed[0].shape[2]
    tiles = sums[0].shape[1]
    width = packed[0].shape[-1]
    rows = far[0].shape[3]
    owner = 2 * expert + half
    block = 4 * expert + shard
    is_near = x == half
    columns = [3 - shard, (shard + 2) % 4, shard + 1 - 2 * (shard % 2), shard]

    def load(i):
        lanes = pl.ds(pl.multiple_of(columns[i] * width, width), width)
        return (
            pltpu.make_async_copy(weights.at[:, :, :, lanes], w_buf[i], in_sem.at[i, 0]),
            pltpu.make_async_copy(fisher.at[:, :, :, lanes], f_buf[i], in_sem.at[i, 1]),
        )

    def pack(i):
        for copy in load(i):
            copy.wait()

        def step(n, carry):
            e, k = n // cap, n % cap
            tile = jnp.minimum(plan[0, (e * 8 + block) * cap + k], tiles - 1)
            share = f_buf[i][e, tile]
            packed[i][e, 0, k] = share * w_buf[i][e, tile]
            packed[i][e, 1, k] = share
            return carry

        lax.fori_loop(0, 2 * cap, step, 0)

    def gather(i, de, dx):
        to_expert, to_x = (expert + de) % 2, (x + dx) % 2
        start = pl.multiple_of(DIRECT + rows * to_x, 16)
        part = packed[i].at[to_expert, :, :, pl.ds(start, rows)]
        target = gathered[i].at[task]
        return part, target, mesh_copy(
            part, target, g_send.at[i, de, dx], g_recv.at[i, task], (to_expert, 2 * expert + to_x, shard)
        )

    def straight(i, de, g):
        to_expert = (expert + de) % 2
        part = packed[i].at[to_expert, :, :, pl.ds(DIRECT * g, DIRECT)]
        target = direct[i % 2][g].at[task]
        return part, target, mesh_copy(
            part, target, n_send.at[i, de, g], n_recv.at[i % 2, g, task], (to_expert, owner, columns[i])
        )

    def start(copy, own, sem):
        part, target, remote = copy
        if own is None:
            remote.start()
        else:
            pl.when(own)(pltpu.make_async_copy(part, target, sem).start)
            pl.when(jnp.logical_not(own))(remote.start)

    def reduced(i):
        return mesh_copy(
            sums[i], far[i].at[x], s_send.at[i], s_recv.at[i, x], (expert, 2 * y + half, columns[i])
        )

    def tell(step):
        return mesh_copy(
            plan_hbm, plans.at[task], p_send.at[step], p_recv.at[task], (expert, (task + step) % 4, shard)
        )

    def come(target, sem):
        return mesh_copy(target, target, p_send.at[0], sem, (1 - expert, task, shard))

    for i in range(4):
        for copy in load(i):
            copy.start()
    get_base = pltpu.make_async_copy(base, base_buf, base_sem)
    get_base.start()
    me = (expert * 4 + task) * 4 + shard
    barrier = pltpu.get_barrier_semaphore()

    def greet(n, carry):
        @pl.when(n != me)
        def _():
            pl.semaphore_signal(barrier, inc=1, device_id=(n // 16, (n // 4) % 4, n % 4), device_id_type=MESH)

        return carry

    lax.fori_loop(0, 32, greet, 0)
    pack(0)
    pl.semaphore_wait(barrier, 31)

    own_plan = pltpu.make_async_copy(plan_hbm, plans.at[task], table_sem.at[0])
    own_plan.start()
    for step in range(1, 4):
        tell(step).start()

    gather_own = jnp.logical_and(expert == y, True)
    near_own = jnp.logical_and(expert == y, is_near)

    def send_far(i):
        for de in range(2):
            for dx in (1, 0):
                start(gather(i, de, dx), gather_own if de == 0 and dx == 0 else None, g_own.at[i])
        for de in range(2):
            start(straight(i, de, 0), None, None)

    def send_near(i):
        for g in range(len(direct[0])):
            for de in range(2):
                start(straight(i, de, g), near_own if i == 3 and de == 0 else None, n_own.at[g])

    send_far(0)
    pack(1)
    send_far(1)
    pack(2)
    send_near(2)
    pack(3)
    send_near(3)

    own_plan.wait()
    for source in range(4):
        pl.when(task != source)(come(plans.at[source], p_recv.at[source]).wait_recv)
    fetch = pltpu.make_async_copy(plans, tables, table_sem.at[1])
    fetch.start()
    fetch.wait()
    blocks = [4 * y + shard, 4 * y + 2 * x + 1 - shard % 2, 4 * y + 2 * x + shard % 2]

    def look(n, carry):
        t, tile = n // tiles, n % tiles
        for which, at in enumerate(blocks):
            slot, found = jnp.int32(0), jnp.int32(0)
            for k in range(cap):
                hit = (tables[t, 0, (expert * 8 + at) * cap + k] == tile).astype(jnp.int32)
                slot = jnp.maximum(slot, hit * k)
                found = jnp.maximum(found, hit)
            slots[which, n] = slot
            live[which, n] = found
        return carry

    lax.fori_loop(0, 4 * tiles, look, 0)

    def kept(which, tile):
        return [
            (slots[which, t * tiles + tile], live[which, t * tiles + tile].astype(jnp.float32)) for t in range(4)
        ]

    def added(ref, which, terms):
        return sum(ref[t, which, s].astype(jnp.float32) * k for t, (s, k) in enumerate(terms))

    for i in range(2):
        for source in range(4):
            own = jnp.logical_and(expert == y, task == source)
            part, target, _ = gather(i, 0, 0)
            pl.when(own)(pltpu.make_async_copy(part, target, g_own.at[i]).wait)
            pl.when(jnp.logical_not(own))(come(gathered[i].at[source], g_recv.at[i, source]).wait_recv)

        def total(tile, carry, i=i):
            terms = kept(0, tile)
            for which in range(2):
                sums[i][which, tile] = added(gathered[i], which, terms).astype(jnp.bfloat16)
            return carry

        lax.fori_loop(0, tiles, total, 0)
        reduced(i).start()

    get_base.wait()

    def settle(at, span, numerator, denominator):
        numerator += PRIOR_WEIGHT * base_buf[at, span].astype(jnp.float32)
        out_buf[at, span] = (numerator / (denominator + PRIOR_WEIGHT)).astype(jnp.bfloat16)

    def deliver(k, first):
        place = (shard + 1 + k) % 2
        group = pl.ds(pl.multiple_of(place * tiles, tiles), tiles)

        def arrived(g, own_too):
            for source in range(4):
                arrive = come(direct[k][g].at[source], n_recv.at[k, g, source])
                if own_too:
                    own = jnp.logical_and(expert == y, task == source)
                    part, target, _ = straight(3, 0, g)
                    pl.when(own)(pltpu.make_async_copy(part, target, n_own.at[g]).wait)
                    pl.when(jnp.logical_not(own))(arrive.wait_recv)
                else:
                    arrive.wait_recv()

        def plain(g):
            span = pl.ds(DIRECT * g, DIRECT)

            def one(tile, carry):
                terms = kept(1 + k, tile)
                settle(place * tiles + tile, span, added(direct[k][g], 0, terms), added(direct[k][g], 1, terms))
                return carry

            lax.fori_loop(0, tiles, one, 0)

        def write(g, count):
            span = pl.ds(DIRECT * g, DIRECT * count)
            return pltpu.make_async_copy(
                out_buf.at[group, span], merged.at[group, span], out_sem.at[k, g]
            )

        groups = len(direct[0])

        @pl.when(is_near)
        def _():
            for g in range(groups):
                if first:
                    arrived(g, k == 1)
                    plain(g)
                    write(g, 1).start()
                else:
                    write(g, 1).wait()

        @pl.when(jnp.logical_not(is_near))
        def _():
            if not first:
                write(0, groups).wait()
                return
            arrived(0, False)
            plain(0)
            for source in range(2):
                come(far[k].at[source], s_recv.at[k, source]).wait_recv()

            def one(tile, carry):
                for source in range(2):
                    settle(
                        place * tiles + tile,
                        pl.ds(DIRECT + rows * source, rows),
                        far[k][source, 0, tile].astype(jnp.float32),
                        far[k][source, 1, tile].astype(jnp.float32),
                    )
                return carry

            lax.fori_loop(0, tiles, one, 0)
            write(0, groups).start()

    deliver(0, True)
    deliver(1, True)
    for step in range(1, 4):
        tell(step).wait_send()
    for i in range(2):
        for de in range(2):
            for dx in range(2):
                remote = gather(i, de, dx)[2]
                if de == 0 and dx == 0:
                    pl.when(jnp.logical_not(gather_own))(remote.wait_send)
                else:
                    remote.wait_send()
            straight(i, de, 0)[2].wait_send()
        reduced(i).wait_send()
    for i in (2, 3):
        for g in range(len(direct[0])):
            for de in range(2):
                remote = straight(i, de, g)[2]
                if i == 3 and de == 0:
                    pl.when(jnp.logical_not(near_own))(remote.wait_send)
                else:
                    remote.wait_send()
    deliver(0, False)
    deliver(1, False)


def fused(plan, weights, fisher, base):
    experts, tiles, _, columns = weights.shape
    width = base.shape[-1]
    cap = plan.shape[1] // 2 // 16
    groups = TILE // DIRECT
    rows = (TILE - DIRECT) // 2
    b16 = lambda *shape: pltpu.VMEM(shape, jnp.bfloat16)
    dma = lambda *shape: pltpu.SemaphoreType.DMA(shape)
    anywhere = pl.BlockSpec(memory_space=pl.ANY)
    scratch = [
        [b16(experts, tiles, TILE, width) for _ in range(4)],
        [b16(experts, tiles, TILE, width) for _ in range(4)],
        [b16(experts, 2, cap, TILE, width) for _ in range(4)],
        [b16(4, 2, cap, rows, width) for _ in range(2)],
        [b16(2, tiles, rows, width) for _ in range(2)],
        [[b16(4, 2, cap, DIRECT, width) for _ in range(groups)] for _ in range(2)],
        [b16(2, 2, tiles, rows, width) for _ in range(2)],
        b16(*base.shape),
        b16(*base.shape),
        pltpu.VMEM((4,) + plan.shape, jnp.int32),
        pltpu.SMEM((4,) + plan.shape, jnp.int32),
        pltpu.SMEM((3, 4 * tiles), jnp.int32),
        pltpu.SMEM((3, 4 * tiles), jnp.int32),
        dma(4, 2), pltpu.SemaphoreType.DMA, dma(2, groups), dma(4), dma(4), dma(2),
        dma(2, 2, 2), dma(2, 4), dma(2), dma(4, 2, groups), dma(2, groups, 4), dma(groups), dma(2), dma(2, 2),
    ]
    return pl.pallas_call(
        fused_body,
        out_shape=jax.ShapeDtypeStruct(base.shape, jnp.bfloat16),
        in_specs=[pl.BlockSpec(memory_space=pltpu.SMEM)] + [anywhere] * 4,
        out_specs=anywhere,
        scratch_shapes=scratch,
        compiler_params=pltpu.CompilerParams(
            has_side_effects=True, collective_id=0, vmem_limit_bytes=60 * 1024 * 1024
        ),
        name="fused",
    )(plan, plan, weights, fisher, base)


def local(weights, fisher, base_weights, tile_list, tile_count):
    experts, tasks, shards = (lax.axis_size(a) for a in ("expert", "task", "shard"))
    expert, task, shard = (lax.axis_index(a) for a in ("expert", "task", "shard"))
    per_block = weights.shape[2] // TILE
    cap = tile_list.shape[-1]
    group = experts * shards // tasks
    block = expert * shards + shard
    slot_number = jnp.arange(cap, dtype=jnp.int32)
    marked = jnp.where(slot_number < tile_count[..., None], tile_list, per_block)

    if (experts, tasks, shards, weights.shape[1]) == (2, 4, 4, 2):
        base = base_weights[0]
        plan = jnp.pad(marked.reshape(1, -1), ((0, 0), (0, marked.size)))
        blocks = base.reshape(-1, TILE, base.shape[-1])
        tiled = (weights.shape[1], per_block, TILE, weights.shape[3])
        return fused(plan, weights.reshape(tiled), fisher.reshape(tiled), blocks).reshape(base.shape)[None]

    own_list = lax.dynamic_index_in_dim(tile_list[0], block, 1, keepdims=False)
    own_count = lax.dynamic_index_in_dim(tile_count[0], block, 1, keepdims=False)
    own_live = (slot_number[None, :] < own_count[:, None]).astype(jnp.int32)
    packed = pack(own_list.reshape(-1), own_live.reshape(-1), weights[0], fisher[0], shards)
    plans = lax.all_gather(marked[0], "task")
    plans = lax.dynamic_index_in_dim(plans, expert, 1, keepdims=False)
    part = lax.dynamic_slice_in_dim(plans, task * group, group, 1)
    hits = part[..., None] == jnp.arange(per_block, dtype=jnp.int32)
    slots = jnp.sum(hits * slot_number[:, None], axis=2).astype(jnp.int32).reshape(-1)
    live = jnp.any(hits, axis=2).astype(jnp.int32).reshape(-1)
    received = exchange(packed, (experts, tasks, shards))
    return merge(slots, live, received, base_weights[0])[None]


def solution(mesh):
    in_specs = (
        P("task", None, ("expert", "shard"), None),
        P("task", None, ("expert", "shard"), None),
        P("expert", "task", "shard"),
        P("task", None, None, None),
        P("task", None, None),
    )
    out_specs = P("expert", "task", "shard")
    return jax.shard_map(local, mesh=mesh, in_specs=in_specs, out_specs=out_specs, check_vma=False)
```
